32 devices in a mesh: grp: 16 (over z, x, core), fsdp: 2 (over y).
Axes of the slice: x: 2, y: 2, z: 4, core: 2. Of those that a mesh axis runs over, the one named last changes fastest.
Arguments:
- tokens: bfloat16 [12288, 3584], P(('grp', 'fsdp')), may hold values from -6 to 6
- target: bfloat16 [12288, 1024], P(('grp', 'fsdp')), may hold values from -6 to 6
- weight: bfloat16 [3584, 1024], P('fsdp'), may hold values from -0.09375 to 0.09375
- factor_a: bfloat16 [3584, 512], P('fsdp'), may hold values from -6 to 6
- factor_b: bfloat16 [512, 1024], replicated, may hold values from -6 to 6
- counts: int32 [256], replicated, may hold values from 1 to 192, 12288 in all
- cand_index: int32 [256, 2], replicated, may hold values from 0 to 511
Outputs:
- update: float32 [3584, 1024], P('fsdp')
- scores: float32 [256], replicated
The draws below stay inside these ranges and needn't reach their ends.
Inputs may be any that keep to these rules, and one draw needn't show every extreme that they name: The counts sum to 12288; candidate i owns the tokens from counts[0] + ... + counts[i-1] on.
All inputs are finite; a program needn't handle non-finite values.
Results may differ from the reference program's by a relative error of at most 0.003.
Values may be sent and summed in bfloat16 or wider, within the bound.
No kernel may reach another device: no remote copies, remote signals or barrier semaphores. Data moves between devices by JAX's collectives and lax.ppermute only.
A program may use at most 64 MiB of HBM per device.

```python
import math
import jax
import jax.numpy as jnp
import numpy as np
from jax import lax

D = 3584
OUT = 1024
POOL = 512
TOK_DEV = 384
CANDS = 256
TOKENS = 12288


def plant(result, rng, smallest, top_value):
    place = [jax.random.randint(jax.random.fold_in(rng, axis), (), 0, length) for axis, length in enumerate(result.shape)]
    widest = result.shape.index(max(result.shape))
    beside = place[:widest] + [(place[widest] + 1) % result.shape[widest]] + place[widest + 1:]
    return result.at[tuple(place)].set(smallest).at[tuple(beside)].set(top_value)


def levels(own_key, shape, pieces, least, largest):
    def one(dim, blocks):
        steps = jax.random.uniform(jax.random.fold_in(jax.random.fold_in(own_key, 6), dim), (blocks,), jnp.float32, least / len(pieces), largest / len(pieces))
        return jnp.repeat(jnp.exp(steps), shape[dim] // blocks).reshape((-1,) + (1,) * (len(shape) - dim - 1))

    level = one(*pieces[0])
    for cut in pieces[1:]:
        level = level * one(*cut)
    return level


def length_profile(amount, total, reach, slope):
    portions = [(1 << 20) // math.isqrt(standing ** slope) + 1 for standing in range(2, amount + 1)]
    rest, holding = total - reach - (amount - 1), [1] * (amount - 1)
    while rest > 0:
        movable = [i for i in range(amount - 1) if holding[i] < reach]
        whole, remaining = sum([portions[i] for i in movable]), rest
        for i in movable:
            extra = min(reach - holding[i], max(1, remaining * portions[i] // whole), rest)
            holding[i] = holding[i] + extra
            rest = rest - extra
    return np.array([reach] + holding)


def ragged(stream_key, count, total, reach, skew):
    if count == 2:
        one = jax.random.randint(stream_key, (), max(1, total - reach), min(reach, total - 1) + 1)
        return jnp.stack([one, total - one])
    lengths = jnp.asarray(length_profile(count, total, reach, skew), jnp.int32)
    twos = (count - 1) // 2
    giver, receiver = lengths[1:1 + 2 * twos:2], lengths[2:2 + 2 * twos:2]
    room = jnp.minimum(giver - 1, reach - receiver)
    passed = jax.random.randint(jax.random.fold_in(stream_key, 1), (twos,), 0, 1 << 20) % (room + 1)
    lengths = lengths.at[1:1 + 2 * twos:2].set(giver - passed).at[2:2 + 2 * twos:2].set(receiver + passed)
    return lengths[jax.random.permutation(jax.random.fold_in(stream_key, 2), count)]


def bell_draw(own_key, dims, deviation, most, split=(), kind=jnp.bfloat16):
    factor_of = levels(own_key, dims, split, -0.22, 0.18) if split else 1.0
    values = jax.random.normal(own_key, dims, jnp.float32) * deviation * factor_of
    return jnp.minimum(jnp.maximum(values, -most), most).astype(kind)


def setup_inputs(seed: int = 0) -> dict:
    splits = jax.random.split(jax.random.key(seed), 8)
    tokens = bell_draw(splits[0], (TOKENS, D), 1.0, 6.0, ((0, 32),))
    target = bell_draw(splits[1], (TOKENS, OUT), 1.0, 6.0, ((0, 32),))
    weight = bell_draw(splits[2], (D, OUT), D ** -0.5, 0.09375, ((0, 2),))
    factor_a = bell_draw(splits[3], (D, POOL), 1.0, 6.0, ((0, 2),))
    factor_b = bell_draw(splits[4], (POOL, OUT), 1.0, 6.0)
    counts = ragged(splits[5], CANDS, TOKENS, 4 * TOKENS // CANDS, 2).astype(jnp.int32)
    cand_index = plant(jax.random.randint(splits[6], (CANDS, 2), 0, POOL), jax.random.fold_in(splits[6], 1), 0, POOL - 1).astype(jnp.int32)
    return {"tokens": tokens, "target": target, "weight": weight, "factor_a": factor_a, "factor_b": factor_b, "counts": counts, "cand_index": cand_index}


def reference(tokens, target, weight, factor_a, factor_b, counts, cand_index):
    noise = 0.5 * D ** (-0.5)
    ends = jnp.cumsum(counts).astype(jnp.int32)
    position = jnp.arange(TOKENS, dtype=jnp.int32)
    owner = jnp.searchsorted(ends, position, side='right').astype(jnp.int32)
    left_index = cand_index[:, 0]
    right_index = cand_index[:, 1]
    tok_a = jnp.take(left_index, owner)
    tok_b = jnp.take(right_index, owner)
    weight_wide = weight.astype(jnp.float32)
    pool_rows = factor_a.T.astype(jnp.float32)
    pool_right = factor_b.astype(jnp.float32)
    blocks = TOKENS // TOK_DEV

    def one_block(items):
        x_rows, t_rows, a_sel, b_sel = items
        x_wide = x_rows.astype(jnp.float32)
        base = jnp.dot(x_wide, weight_wide, precision=lax.Precision.HIGHEST)
        a_rows = jnp.take(pool_rows, a_sel, axis=0)
        score = lax.optimization_barrier(jnp.sum(x_wide * a_rows, axis=1))
        b_rows = jnp.take(pool_right, b_sel, axis=0)
        output = base + noise * score[:, None] * b_rows
        diff = output - t_rows.astype(jnp.float32)
        return lax.optimization_barrier(jnp.mean(diff * diff, axis=1))
    loss = lax.map(one_block, (tokens.reshape(blocks, TOK_DEV, D), target.reshape(blocks, TOK_DEV, OUT), tok_a.reshape(blocks, TOK_DEV), tok_b.reshape(blocks, TOK_DEV))).reshape(TOKENS)
    totals = jax.ops.segment_sum(loss, owner, num_segments=CANDS)
    fitness = -totals / counts.astype(jnp.float32)
    middle = jnp.mean(fitness)
    spread = jnp.mean((fitness - middle) ** 2)
    scores = (fitness - middle) / jnp.sqrt(spread + 1e-06)
    columns = jnp.take(factor_a, left_index, axis=1).astype(jnp.float32)
    scaled = (columns * scores[None, :]).astype(jnp.bfloat16)
    right_rows = jnp.take(factor_b, right_index, axis=0).astype(jnp.float32)
    update = jnp.dot(scaled.astype(jnp.float32), right_rows, precision=lax.Precision.HIGHEST) / jnp.sqrt(jnp.float32(CANDS))
    return (update, scores)
```

```python
import functools

import jax
import jax.numpy as jnp
from jax import lax
from jax.experimental import pallas as pl
from jax.experimental.pallas import tpu as pltpu
from jax.sharding import PartitionSpec as P

AXES = ("grp", "fsdp")
f32 = jnp.float32
bf16 = jnp.bfloat16
PIECES = 8


def pack_kernel(rows_ref, left_ref, *refs):
    del rows_ref
    weights, factors, outs = refs[:4], refs[4:8], refs[8:]
    pool = factors[0].shape[1]
    cands = left_ref.shape[1]
    ids = lax.broadcasted_iota(jnp.int32, (pool, cands), 0)
    selector = (ids == left_ref[...]).astype(f32).astype(bf16)
    for w, a, o in zip(weights, factors, outs):
        width = w.shape[1]
        o[:, :width] = w[...]
        o[:, width:] = jnp.dot(a[...], selector, preferred_element_type=f32).astype(bf16)


def pack(blocks, left, weight, factor_a, height):
    width, pool, cands = weight.shape[1], factor_a.shape[1], left.shape[1]

    def at(k, columns):
        return pl.BlockSpec((height, columns), lambda i, t: (t[k], 0))

    return pl.pallas_call(
        pack_kernel,
        grid_spec=pltpu.PrefetchScalarGridSpec(
            num_scalar_prefetch=1,
            grid=(1,),
            in_specs=[pl.BlockSpec((1, cands), lambda i, t: (0, 0))]
            + [at(k, width) for k in range(4)]
            + [at(k, pool) for k in range(4)],
            out_specs=[pl.BlockSpec((height, width + cands), lambda i, t: (0, 0))] * 4,
        ),
        out_shape=[jax.ShapeDtypeStruct((height, width + cands), bf16)] * 4,
        name="pack",
    )(blocks, left, *([weight] * 4), *([factor_a] * 4))


def loss_kernel(noise, count, at_ref, x_ref, base_ref, sc_ref, target_ref, right_ref, hot_ref, *refs):
    pieces, out_ref, held, sem = refs[:count], refs[count], refs[count + 1], refs[count + 2]
    height = pieces[0].shape[0]
    copies = []
    for k in range(count):
        start = pl.multiple_of(at_ref[1 + k] * height, 16)
        copies.append(pltpu.make_async_copy(pieces[k], held.at[pl.ds(start, height)], sem.at[k]))
    for c in copies:
        c.start()
    for c in copies:
        c.wait()
    rows, width = target_ref.shape
    total = None
    step = 128
    for r in range(0, rows, step):
        s = slice(r, r + step)
        acc = jnp.dot(x_ref[s, :], held[...], preferred_element_type=f32)
        hot = hot_ref[s, :].astype(f32)
        picked = jnp.sum(hot * (acc[:, width:] + sc_ref[s, :]), axis=1, keepdims=True) * noise
        diff = acc[:, :width] + base_ref[s, :] + picked * right_ref[s, :].astype(f32) - target_ref[s, :].astype(f32)
        loss = jnp.sum(diff * diff, axis=1, keepdims=True) * (1.0 / width)
        part = jnp.sum(hot * loss, axis=0, keepdims=True)
        total = part if total is None else total + part
    out_ref[...] = jnp.broadcast_to(total, out_ref.shape)


def losses(where, x, base, sc, target, right, hot, pieces, devices, noise):
    rows, width = target.shape
    half, cands = x.shape[1] // 2, hot.shape[1]
    count = len(pieces)

    def whole(a):
        return pl.BlockSpec(a.shape, lambda i, t: (0, 0))

    return pl.pallas_call(
        functools.partial(loss_kernel, noise, count),
        grid_spec=pltpu.PrefetchScalarGridSpec(
            num_scalar_prefetch=1,
            grid=(1,),
            in_specs=[pl.BlockSpec((rows, half), lambda i, t: (0, t[0]))]
            + [whole(a) for a in (base, sc, target, right, hot)]
            + [pl.BlockSpec(memory_space=pltpu.HBM)] * count,
            out_specs=pl.BlockSpec((devices, cands), lambda i, t: (0, 0)),
            scratch_shapes=[
                pltpu.VMEM((half, width + cands), bf16),
                pltpu.SemaphoreType.DMA((count,)),
            ],
        ),
        out_shape=jax.ShapeDtypeStruct((devices, cands), f32),
        name="losses",
    )(where, x, base, sc, target, right, hot, *pieces)


def update_kernel(parts_ref, counts_ref, columns_ref, rows_ref, update_ref, scores_ref):
    cands = counts_ref.shape[1]
    totals = jnp.sum(parts_ref[...], axis=0, keepdims=True)
    fitness = -totals / counts_ref[...].astype(f32)
    middle = jnp.sum(fitness, axis=1, keepdims=True) / cands
    spread = jnp.sum((fitness - middle) ** 2, axis=1, keepdims=True) / cands
    scores = (fitness - middle) / jnp.sqrt(spread + 1e-06)
    scores_ref[...] = scores
    scaled = (columns_ref[...].astype(f32) * scores).astype(bf16)
    update_ref[...] = jnp.dot(scaled, rows_ref[...], preferred_element_type=f32) * (1.0 / cands**0.5)


def update_of(parts, counts, columns, rows):
    depth, cands = columns.shape
    width = rows.shape[1]
    step = next(s for s in (256, 224, 128, 64, 16, depth) if depth % s == 0)
    return pl.pallas_call(
        update_kernel,
        grid=(depth // step,),
        in_specs=[
            pl.BlockSpec(parts.shape, lambda i: (0, 0)),
            pl.BlockSpec((1, cands), lambda i: (0, 0)),
            pl.BlockSpec((step, cands), lambda i: (i, 0)),
            pl.BlockSpec((cands, width), lambda i: (0, 0)),
        ],
        out_specs=[
            pl.BlockSpec((step, width), lambda i: (i, 0)),
            pl.BlockSpec((1, cands), lambda i: (0, 0)),
        ],
        out_shape=[
            jax.ShapeDtypeStruct((depth, width), f32),
            jax.ShapeDtypeStruct((1, cands), f32),
        ],
        name="update",
    )(parts, counts, columns, rows)


def hop(value, bit, devices):
    return lax.ppermute(value, AXES, [(i, i ^ bit) for i in range(devices)])


def per_device(groups, parts, tokens, target, weight, factor_a, factor_b, counts, cand_index):
    devices = groups * parts
    rows, full = tokens.shape
    depth, width = weight.shape
    pool, cands = factor_a.shape[1], counts.shape[0]
    noise = 0.5 * full ** (-0.5)
    left, right = cand_index[:, 0], cand_index[:, 1]
    grp, fsdp = lax.axis_index("grp"), lax.axis_index("fsdp")
    square = parts == 2 and groups % 8 == 0 and depth % (2 * PIECES * 16) == 0
    if square:
        height = depth // (2 * PIECES)
        core, spot = grp % 2, (grp // 2) % 4
        mine = jnp.stack([spot, spot + 4, 3 - spot, 7 - spot])
        first, second, third, fourth = pack(
            (2 * mine + core).astype(jnp.int32), left[None, :], weight, factor_a, height
        )
        y1, y2, y3, y4 = (hop(v, 1, devices) for v in (first, second, third, fourth))
        x1, z1 = hop(y1, 4, devices), hop(y1, 8, devices)
        x2, z2 = hop(y2, 4, devices), hop(y2, 8, devices)
        own = [y1, y2, x1, z1, y3, y4, x2, z2]
        ids = [spot, spot + 4, spot ^ 1, spot ^ 2, 3 - spot, 7 - spot, (spot ^ 1) + 4, (spot ^ 2) + 4]
        other = [hop(v, 2, devices) for v in own]
        where = jnp.stack(
            [1 - fsdp] + [2 * i + core for i in ids] + [2 * i + 1 - core for i in ids]
        ).astype(jnp.int32)

    cand_ids = jnp.arange(cands, dtype=jnp.int32)
    ends = jnp.sum(jnp.where(cand_ids[:, None] <= cand_ids[None, :], counts[:, None], 0), axis=0)
    position = (grp * parts + fsdp) * rows + jnp.arange(rows, dtype=jnp.int32)
    hot = (position[:, None] >= (ends - counts)[None, :]) & (position[:, None] < ends[None, :])
    hot = hot.astype(bf16)
    pool_ids = jnp.arange(pool, dtype=jnp.int32)
    columns = jnp.dot(factor_a, (pool_ids[:, None] == left[None, :]).astype(bf16), preferred_element_type=f32).astype(bf16)
    chosen = jnp.dot((right[:, None] == pool_ids[None, :]).astype(bf16), factor_b, preferred_element_type=f32).astype(bf16)
    right_rows = jnp.dot(hot, chosen, preferred_element_type=f32).astype(bf16)

    if square:
        near = lax.dynamic_slice_in_dim(tokens, fsdp * depth, depth, axis=1)
        base = jnp.dot(near, weight, preferred_element_type=f32)
        sc = jnp.dot(near, columns, preferred_element_type=f32)
        sums = losses(where, tokens, base, sc, target, right_rows, hot, own + other, devices, noise)
    else:
        all_weight = lax.all_gather(weight, "fsdp", axis=0, tiled=True)
        all_columns = lax.all_gather(columns, "fsdp", axis=0, tiled=True)
        base = jnp.dot(tokens, all_weight, preferred_element_type=f32)
        sc = jnp.dot(tokens, all_columns, preferred_element_type=f32)
        owned = hot.astype(f32)
        picked = noise * jnp.sum(owned * sc, axis=1)
        diff = base + picked[:, None] * right_rows.astype(f32) - target.astype(f32)
        loss = jnp.mean(diff * diff, axis=1)
        sums = jnp.broadcast_to(jnp.sum(owned * loss[:, None], axis=0)[None, :], (devices, cands))
    spread = lax.all_to_all(sums, AXES, split_axis=0, concat_axis=0, tiled=True)
    update, scores = update_of(spread, counts[None, :], columns, chosen)
    return update, scores[0]


def solution(mesh):
    in_specs = (
        P(AXES, None),
        P(AXES, None),
        P("fsdp", None),
        P("fsdp", None),
        P(),
        P(),
        P(),
    )
    return jax.shard_map(
        functools.partial(per_device, mesh.shape["grp"], mesh.shape["fsdp"]),
        mesh=mesh,
        in_specs=in_specs,
        out_specs=(P("fsdp", None), P()),
        check_vma=False,
    )
```

```python
import functools

import jax
import jax.numpy as jnp
from jax import lax
from jax.experimental import pallas as pl
from jax.experimental.pallas import tpu as pltpu
from jax.sharding import PartitionSpec as P


AXES = ("grp", "fsdp")
f32 = jnp.float32
bf16 = jnp.bfloat16
PIECES = 8


def turned(row, height):
    return jnp.transpose(jnp.broadcast_to(row.astype(f32), (height, row.shape[1])))


def matches(row, pool):
    ids = lax.broadcasted_iota(jnp.int32, (pool, row.shape[1]), 0)
    return (ids == row).astype(f32).astype(bf16)


def pack_kernel(order, index_ref, weight_ref, factor_ref, *refs):
    outs, factors, w_sem, a_sem = refs[:-3], refs[-3], refs[-2], refs[-1]
    height, width = outs[0].shape[0], weight_ref.shape[1]
    copies = []
    for k, (out, block) in enumerate(zip(outs, order())):
        rows = pl.ds(pl.multiple_of(block * height, 16), height)
        a = pltpu.make_async_copy(factor_ref.at[rows], factors.at[k], a_sem.at[k])
        w = pltpu.make_async_copy(weight_ref.at[rows], out.at[:, pl.ds(0, width)], w_sem.at[k])
        a.start()
        w.start()
        copies.append((a, w))
    selector = matches(index_ref[0:1, :], factor_ref.shape[1])
    for k, (out, (a, w)) in enumerate(zip(outs, copies)):
        a.wait()
        out[:, width:] = jnp.dot(factors[k], selector, preferred_element_type=f32).astype(bf16)
    for _, w in copies:
        w.wait()


def vmem():
    return pl.BlockSpec(memory_space=pltpu.VMEM)


def hbm():
    return pl.BlockSpec(memory_space=pltpu.HBM)


def in_hbm(*arrays):
    return [pltpu.with_memory_space_constraint(a, pltpu.HBM) for a in arrays]


def params(mib):
    return pltpu.CompilerParams(vmem_limit_bytes=mib << 20)


def pack(order, count, index, weight, factor_a, height):
    width, pool, cands = weight.shape[1], factor_a.shape[1], index.shape[1]
    return pl.pallas_call(
        functools.partial(pack_kernel, order),
        in_specs=[vmem(), hbm(), hbm()],
        out_specs=[vmem()] * count,
        out_shape=[jax.ShapeDtypeStruct((height, width + cands), bf16)] * count,
        scratch_shapes=[
            pltpu.VMEM((count, height, pool), bf16),
            pltpu.SemaphoreType.DMA((count,)),
            pltpu.SemaphoreType.DMA((count,)),
        ],
        compiler_params=params(8),
        name="pack",
    )(index, *in_hbm(weight, factor_a))


def near_kernel(
    index_ref, counts_ref, tokens_ref, weight_ref, factor_ref, rights_ref, target_ref,
    far_ref, base_ref, sc_ref, hot_ref, right_ref, columns_ref, chosen_ref,
    x, w, a, b, t, sem,
):
    fsdp = lax.axis_index("fsdp")
    device = lax.axis_index("grp") * lax.axis_size("fsdp") + fsdp
    rows, depth = far_ref.shape
    cands = counts_ref.shape[1]
    pool = factor_ref.shape[1]
    near = pl.ds(pl.multiple_of(fsdp * depth, 128), depth)
    other = pl.ds(pl.multiple_of((1 - fsdp) * depth, 128), depth)
    pairs = [
        (factor_ref, a), (rights_ref, b), (tokens_ref.at[:, near], x), (weight_ref, w),
        (target_ref, t), (tokens_ref.at[:, other], far_ref),
    ]
    copies = [pltpu.make_async_copy(s, d, sem.at[k]) for k, (s, d) in enumerate(pairs)]
    for c in copies:
        c.start()
    along = lax.broadcasted_iota(jnp.int32, (cands, cands), 0)
    across = lax.broadcasted_iota(jnp.int32, (cands, cands), 1)
    ends = jnp.sum(jnp.where(along <= across, turned(counts_ref[...], cands), 0.0), axis=0, keepdims=True)
    begins = ends - counts_ref[...].astype(f32)
    position = (device * rows + lax.broadcasted_iota(jnp.int32, (rows, cands), 0)).astype(f32)
    hot = jnp.where((position >= begins) & (position < ends), 1.0, 0.0).astype(bf16)
    hot_ref[...] = hot
    copies[0].wait()
    columns_ref[...] = jnp.dot(a[...], matches(index_ref[0:1, :], pool), preferred_element_type=f32).astype(bf16)
    copies[1].wait()
    chosen = lax.dot_general(
        matches(index_ref[1:2, :], pool), b[...], (((0,), (0,)), ((), ())), preferred_element_type=f32
    ).astype(bf16)
    chosen_ref[...] = chosen
    right_ref[...] = jnp.dot(hot, chosen, preferred_element_type=f32).astype(bf16)
    copies[2].wait()
    sc_ref[...] = jnp.dot(x[...], columns_ref[...], preferred_element_type=f32)
    copies[3].wait()
    copies[4].wait()
    base_ref[...] = jnp.dot(x[...], w[...], preferred_element_type=f32) - t[...].astype(f32)
    copies[5].wait()


def near_half(index, counts, tokens, weight, factor_a, factor_b, target):
    rows, width = target.shape
    depth, cands, pool = weight.shape[0], counts.shape[1], factor_a.shape[1]

    def shaped(*shape, dtype=bf16):
        return jax.ShapeDtypeStruct(shape, dtype)

    return pl.pallas_call(
        near_kernel,
        in_specs=[vmem(), vmem()] + [hbm()] * 5,
        out_specs=[vmem()] * 7,
        out_shape=[
            shaped(rows, depth), shaped(rows, width, dtype=f32), shaped(rows, cands, dtype=f32),
            shaped(rows, cands), shaped(rows, width), shaped(depth, cands), shaped(cands, width),
        ],
        scratch_shapes=[
            pltpu.VMEM((rows, depth), bf16), pltpu.VMEM((depth, width), bf16), pltpu.VMEM((depth, pool), bf16),
            pltpu.VMEM((pool, width), bf16), pltpu.VMEM((rows, width), bf16), pltpu.SemaphoreType.DMA((6,)),
        ],
        compiler_params=params(28),
        cost_estimate=pl.CostEstimate(
            flops=2 * rows * depth * (width + cands) * 4, bytes_accessed=12 << 20, transcendentals=0
        ),
        name="near",
    )(index, counts, *in_hbm(tokens, weight, factor_a, factor_b, target))


def loss_kernel(noise, order, x_ref, base_ref, sc_ref, right_ref, hot_ref, *refs):
    pieces, out_ref, held = refs[:-2], refs[-2], refs[-1]
    height = pieces[0].shape[0]
    for piece, block in zip(pieces, order()):
        held[pl.ds(pl.multiple_of(block * height, 16), height), :] = piece[...]
    rows, width = base_ref.shape
    total = None
    step = 128
    for r in range(0, rows, step):
        s = slice(r, r + step)
        acc = jnp.dot(x_ref[s, :], held[...], preferred_element_type=f32)
        hot = hot_ref[s, :].astype(f32)
        picked = jnp.sum(hot * (acc[:, width:] + sc_ref[s, :]), axis=1, keepdims=True) * noise
        diff = acc[:, :width] + base_ref[s, :] + picked * right_ref[s, :].astype(f32)
        loss = jnp.sum(diff * diff, axis=1, keepdims=True) * (1.0 / width)
        part = jnp.sum(hot * loss, axis=0, keepdims=True)
        total = part if total is None else total + part
    out_ref[...] = jnp.broadcast_to(total[None], out_ref.shape)


def losses(noise, order, x, base, sc, right, hot, pieces, devices):
    depth, width, cands = x.shape[1], base.shape[1], hot.shape[1]
    return pl.pallas_call(
        functools.partial(loss_kernel, noise, order),
        in_specs=[vmem()] * (5 + len(pieces)),
        out_specs=vmem(),
        out_shape=jax.ShapeDtypeStruct((devices, 1, cands), f32),
        scratch_shapes=[pltpu.VMEM((depth, width + cands), bf16)],
        compiler_params=params(20),
        name="losses",
    )(x, base, sc, right, hot, *pieces)


def update_kernel(step, parts_ref, counts_ref, columns_ref, chosen_ref, update_ref, scores_ref, held, sem):
    cands = counts_ref.shape[1]
    totals = jnp.sum(parts_ref[...], axis=0)
    fitness = -totals / counts_ref[...].astype(f32)
    middle = jnp.sum(fitness, axis=1, keepdims=True) / cands
    spread = jnp.sum((fitness - middle) ** 2, axis=1, keepdims=True) / cands
    scores = (fitness - middle) / jnp.sqrt(spread + 1e-06)
    scores_ref[...] = scores
    copies = []
    for k in range(columns_ref.shape[0] // step):
        s = pl.ds(k * step, step)
        scaled = (columns_ref[s, :].astype(f32) * scores).astype(bf16)
        held[s, :] = jnp.dot(scaled, chosen_ref[...], preferred_element_type=f32) * (1.0 / cands**0.5)
        c = pltpu.make_async_copy(held.at[s], update_ref.at[s], sem.at[k])
        c.start()
        copies.append(c)
    for c in copies:
        c.wait()


def update_of(parts, counts, columns, chosen):
    depth, cands = columns.shape
    width = chosen.shape[1]
    step = next(s for s in (128, 64, 32, 16, depth) if depth % s == 0)
    return pl.pallas_call(
        functools.partial(update_kernel, step),
        in_specs=[vmem()] * 4,
        out_specs=[hbm(), vmem()],
        out_shape=[jax.ShapeDtypeStruct((depth, width), f32), jax.ShapeDtypeStruct((1, cands), f32)],
        scratch_shapes=[pltpu.VMEM((depth, width), f32), pltpu.SemaphoreType.DMA((depth // step,))],
        compiler_params=params(20),
        name="update",
    )(parts, counts, columns, chosen)


def hop(value, bit, devices):
    return lax.ppermute(value, AXES, [(i, i ^ bit) for i in range(devices)])


def place():
    grp = lax.axis_index("grp")
    return jnp.bitwise_and(grp, 1), jnp.bitwise_and(jnp.right_shift(grp, 1), 3)


def sent():
    core, spot = place()
    return [2 * i + core for i in (spot, spot + 4, 3 - spot, 7 - spot)]


def arrived():
    core, spot = place()
    x, z = jnp.bitwise_xor(spot, 1), jnp.bitwise_xor(spot, 2)
    ids = [spot, spot + 4, x, z, 3 - spot, 7 - spot, x + 4, z + 4]
    return [2 * i + core for i in ids] + [2 * i + 1 - core for i in ids]


def per_device(groups, parts, tokens, target, weight, factor_a, factor_b, counts, cand_index):
    return compute(groups, parts, tokens, target, weight, factor_a, factor_b, counts, cand_index)


def compute(groups, parts, tokens, target, weight, factor_a, factor_b, counts, cand_index):
    devices = groups * parts
    rows, full = tokens.shape
    depth = weight.shape[0]
    cands = counts.shape[0]
    noise = 0.5 * full ** (-0.5)
    index = cand_index.T
    if parts == 2 and groups % 8 == 0 and depth % (2 * PIECES * 16) == 0:
        height = depth // (2 * PIECES)
        first, second, third, fourth = pack(sent, 4, index, weight, factor_a, height)
        y1, y2 = hop(first, 1, devices), hop(second, 1, devices)
        y3, y4 = hop(third, 1, devices), hop(fourth, 1, devices)
        x1, z1 = hop(y1, 4, devices), hop(y1, 8, devices)
        x2, z2 = hop(y2, 4, devices), hop(y2, 8, devices)
        own = [y1, y2, x1, z1, y3, y4, x2, z2]
        swapped = [hop(v, 2, devices) for v in own]
        far, base, sc, hot, right_rows, columns, chosen = near_half(
            index, counts[None, :], tokens, weight, factor_a, factor_b, target
        )
        sums = losses(noise, arrived, far, base, sc, right_rows, hot, own + swapped, devices)
    else:
        left, right = cand_index[:, 0], cand_index[:, 1]
        cand_ids = jnp.arange(cands, dtype=jnp.int32)
        ends = jnp.sum(jnp.where(cand_ids[:, None] <= cand_ids[None, :], counts[:, None], 0), axis=0)
        position = lax.axis_index(AXES) * rows + jnp.arange(rows, dtype=jnp.int32)
        hot = (position[:, None] >= (ends - counts)[None, :]) & (position[:, None] < ends[None, :])
        owned = hot.astype(f32)
        columns = jnp.take(factor_a, left, axis=1)
        chosen = jnp.take(factor_b, right, axis=0)
        right_rows = jnp.dot(hot.astype(bf16), chosen, preferred_element_type=f32)
        all_weight = lax.all_gather(weight, "fsdp", axis=0, tiled=True)
        all_columns = lax.all_gather(columns, "fsdp", axis=0, tiled=True)
        base = jnp.dot(tokens, all_weight, preferred_element_type=f32)
        sc = jnp.dot(tokens, all_columns, preferred_element_type=f32)
        picked = noise * jnp.sum(owned * sc, axis=1)
        diff = base + picked[:, None] * right_rows - target.astype(f32)
        loss = jnp.mean(diff * diff, axis=1)
        sums = jnp.broadcast_to(jnp.sum(owned * loss[:, None], axis=0)[None, None, :], (devices, 1, cands))
    spread = lax.all_to_all(sums, AXES, split_axis=0, concat_axis=0, tiled=True)
    update, scores = update_of(spread, counts[None, :], columns, chosen)
    return update, scores[0]


def solution(mesh):
    in_specs = (
        P(AXES, None),
        P(AXES, None),
        P("fsdp", None),
        P("fsdp", None),
        P(),
        P(),
        P(),
    )
    return jax.shard_map(
        functools.partial(per_device, mesh.shape["grp"], mesh.shape["fsdp"]),
        mesh=mesh,
        in_specs=in_specs,
        out_specs=(P("fsdp", None), P()),
        check_vma=False,
    )
```

```python
import functools

import jax
import jax.numpy as jnp
from jax import lax
from jax.experimental import pallas as pl
from jax.experimental.pallas import tpu as pltpu
from jax.sharding import PartitionSpec as P


AXES = ("grp", "fsdp")
f32 = jnp.float32
bf16 = jnp.bfloat16
PIECES = 8
SKEW = 0


def turned(row, height):
    return jnp.transpose(jnp.broadcast_to(row.astype(f32), (height, row.shape[1])))


def matches(row, pool):
    ids = lax.broadcasted_iota(jnp.int32, (pool, row.shape[1]), 0)
    return (ids == row).astype(f32).astype(bf16)


def pack_kernel(order, index_ref, weight_ref, factor_ref, *refs):
    outs, factors, index, w_sem, a_sem, i_sem = refs[:-5], *refs[-5:]
    width = weight_ref.shape[1]
    first = pltpu.make_async_copy(index_ref, index, i_sem)
    first.start()
    copies = []
    for k, (out, start) in enumerate(zip(outs, order())):
        height = out.shape[0]
        rows = pl.ds(pl.multiple_of(start, 16), height)
        a = pltpu.make_async_copy(factor_ref.at[rows], factors.at[k, pl.ds(0, height)], a_sem.at[k])
        w = pltpu.make_async_copy(weight_ref.at[rows], out.at[:, pl.ds(0, width)], w_sem.at[k])
        a.start()
        w.start()
        copies.append((a, w))
    first.wait()
    selector = matches(index[0:1, :], factor_ref.shape[1])
    for k, (out, (a, w)) in enumerate(zip(outs, copies)):
        a.wait()
        out[:, width:] = jnp.dot(factors[k, : out.shape[0]], selector, preferred_element_type=f32).astype(bf16)
    for _, w in copies:
        w.wait()


def vmem():
    return pl.BlockSpec(memory_space=pltpu.VMEM)


def hbm():
    return pl.BlockSpec(memory_space=pltpu.HBM)


def in_hbm(*arrays):
    return [pltpu.with_memory_space_constraint(a, pltpu.HBM) for a in arrays]


def params(mib):
    return pltpu.CompilerParams(vmem_limit_bytes=mib << 20)


def pack(order, heights, index, weight, factor_a):
    count = len(heights)
    width, pool, cands = weight.shape[1], factor_a.shape[1], index.shape[1]
    return pl.pallas_call(
        functools.partial(pack_kernel, order),
        in_specs=[hbm()] * 3,
        out_specs=[vmem()] * count,
        out_shape=[jax.ShapeDtypeStruct((h, width + cands), bf16) for h in heights],
        scratch_shapes=[
            pltpu.VMEM((count, max(heights), pool), bf16),
            pltpu.VMEM(index.shape, jnp.int32),
            pltpu.SemaphoreType.DMA((count,)),
            pltpu.SemaphoreType.DMA((count,)),
            pltpu.SemaphoreType.DMA,
        ],
        compiler_params=params(8),
        name="pack",
    )(*in_hbm(index, weight, factor_a))


def near_kernel(
    index_ref, counts_ref, tokens_ref, weight_ref, factor_ref, rights_ref, target_ref,
    far_ref, base_ref, sc_ref, hot_ref, right_ref, columns_ref, chosen_ref,
    x, w, a, b, t, sem,
):
    fsdp = lax.axis_index("fsdp")
    device = lax.axis_index("grp") * lax.axis_size("fsdp") + fsdp
    rows, depth = far_ref.shape
    cands = counts_ref.shape[1]
    pool = factor_ref.shape[1]
    near = pl.ds(pl.multiple_of(fsdp * depth, 128), depth)
    other = pl.ds(pl.multiple_of((1 - fsdp) * depth, 128), depth)
    pairs = [
        (factor_ref, a), (rights_ref, b), (tokens_ref.at[:, near], x), (weight_ref, w),
        (target_ref, t), (tokens_ref.at[:, other], far_ref),
    ]
    copies = [pltpu.make_async_copy(s, d, sem.at[k]) for k, (s, d) in enumerate(pairs)]
    for c in copies:
        c.start()
    along = lax.broadcasted_iota(jnp.int32, (cands, cands), 0)
    across = lax.broadcasted_iota(jnp.int32, (cands, cands), 1)
    ends = jnp.sum(jnp.where(along <= across, turned(counts_ref[...], cands), 0.0), axis=0, keepdims=True)
    begins = ends - counts_ref[...].astype(f32)
    position = (device * rows + lax.broadcasted_iota(jnp.int32, (rows, cands), 0)).astype(f32)
    hot = jnp.where((position >= begins) & (position < ends), 1.0, 0.0).astype(bf16)
    hot_ref[...] = hot
    copies[0].wait()
    columns_ref[...] = jnp.dot(a[...], matches(index_ref[0:1, :], pool), preferred_element_type=f32).astype(bf16)
    copies[1].wait()
    chosen = lax.dot_general(
        matches(index_ref[1:2, :], pool), b[...], (((0,), (0,)), ((), ())), preferred_element_type=f32
    ).astype(bf16)
    chosen_ref[...] = chosen
    right_ref[...] = jnp.dot(hot, chosen, preferred_element_type=f32).astype(bf16)
    copies[2].wait()
    sc_ref[...] = jnp.dot(x[...], columns_ref[...], preferred_element_type=f32)
    copies[3].wait()
    copies[4].wait()
    base_ref[...] = jnp.dot(x[...], w[...], preferred_element_type=f32) - t[...].astype(f32)
    copies[5].wait()


def near_half(index, counts, tokens, weight, factor_a, factor_b, target):
    rows, width = target.shape
    depth, cands, pool = weight.shape[0], counts.shape[1], factor_a.shape[1]

    def shaped(*shape, dtype=bf16):
        return jax.ShapeDtypeStruct(shape, dtype)

    return pl.pallas_call(
        near_kernel,
        in_specs=[vmem(), vmem()] + [hbm()] * 5,
        out_specs=[vmem()] * 7,
        out_shape=[
            shaped(rows, depth), shaped(rows, width, dtype=f32), shaped(rows, cands, dtype=f32),
            shaped(rows, cands), shaped(rows, width), shaped(depth, cands), shaped(cands, width),
        ],
        scratch_shapes=[
            pltpu.VMEM((rows, depth), bf16), pltpu.VMEM((depth, width), bf16), pltpu.VMEM((depth, pool), bf16),
            pltpu.VMEM((pool, width), bf16), pltpu.VMEM((rows, width), bf16), pltpu.SemaphoreType.DMA((6,)),
        ],
        compiler_params=params(28),
        cost_estimate=pl.CostEstimate(
            flops=2 * rows * depth * (width + cands) * 4, bytes_accessed=12 << 20, transcendentals=0
        ),
        name="near",
    )(index, counts, *in_hbm(tokens, weight, factor_a, factor_b, target))


def stack(pieces, blocks, held):
    height = pieces[0].shape[0]
    for piece, block in zip(pieces, blocks):
        held[pl.ds(pl.multiple_of(block * height, 16), height), :] = piece[...]


def middle_kernel(order, x_ref, base_ref, sc_ref, *refs):
    pieces, base_out, sc_out, held = refs[:-3], *refs[-3:]
    stack(pieces, order(), held)
    rows, width = base_ref.shape
    half = held.shape[0]
    step = 128
    for r in range(0, rows, step):
        s = slice(r, r + step)
        acc = jnp.dot(x_ref[s, :half], held[...], preferred_element_type=f32)
        base_out[s, :] = base_ref[s, :] + acc[:, :width]
        sc_out[s, :] = sc_ref[s, :] + acc[:, width:]


def middle(order, x, base, sc, pieces):
    depth, columns = x.shape[1], base.shape[1] + sc.shape[1]
    return pl.pallas_call(
        functools.partial(middle_kernel, order),
        in_specs=[vmem()] * (3 + len(pieces)),
        out_specs=[vmem()] * 2,
        out_shape=[jax.ShapeDtypeStruct(base.shape, f32), jax.ShapeDtypeStruct(sc.shape, f32)],
        scratch_shapes=[pltpu.VMEM((sum(p.shape[0] for p in pieces), columns), bf16)],
        compiler_params=params(20),
        cost_estimate=pl.CostEstimate(
            flops=4 * x.shape[0] * depth * columns, bytes_accessed=4 << 20, transcendentals=0
        ),
        name="middle",
    )(x, base, sc, *pieces)


def loss_kernel(noise, order, x_ref, base_ref, sc_ref, right_ref, hot_ref, *refs):
    pieces, out_ref, held = refs[:-2], refs[-2], refs[-1]
    stack(pieces, order(), held)
    rows, width = base_ref.shape
    half = held.shape[0]
    total = None
    step = 128
    for r in range(0, rows, step):
        s = slice(r, r + step)
        acc = jnp.dot(x_ref[s, x_ref.shape[1] - half :], held[...], preferred_element_type=f32)
        hot = hot_ref[s, :].astype(f32)
        picked = jnp.sum(hot * (acc[:, width:] + sc_ref[s, :]), axis=1, keepdims=True) * noise
        diff = acc[:, :width] + base_ref[s, :] + picked * right_ref[s, :].astype(f32)
        loss = jnp.sum(diff * diff, axis=1, keepdims=True) * (1.0 / width)
        part = jnp.sum(hot * loss, axis=0, keepdims=True)
        total = part if total is None else total + part
    out_ref[...] = jnp.broadcast_to(total[None], out_ref.shape)


def losses(noise, order, x, base, sc, right, hot, pieces, devices):
    width, cands = base.shape[1], hot.shape[1]
    return pl.pallas_call(
        functools.partial(loss_kernel, noise, order),
        in_specs=[vmem()] * (5 + len(pieces)),
        out_specs=vmem(),
        out_shape=jax.ShapeDtypeStruct((devices, 1, cands), f32),
        scratch_shapes=[pltpu.VMEM((sum(p.shape[0] for p in pieces), width + cands), bf16)],
        compiler_params=params(20),
        name="losses",
    )(x, base, sc, right, hot, *pieces)


def update_kernel(step, parts_ref, counts_ref, columns_ref, chosen_ref, update_ref, scores_ref, held, sem):
    cands = counts_ref.shape[1]
    totals = jnp.sum(parts_ref[...], axis=0)
    fitness = -totals / counts_ref[...].astype(f32)
    middle = jnp.sum(fitness, axis=1, keepdims=True) / cands
    spread = jnp.sum((fitness - middle) ** 2, axis=1, keepdims=True) / cands
    scores = (fitness - middle) / jnp.sqrt(spread + 1e-06)
    scores_ref[...] = scores
    copies = []
    for k in range(columns_ref.shape[0] // step):
        s = pl.ds(k * step, step)
        scaled = (columns_ref[s, :].astype(f32) * scores).astype(bf16)
        held[s, :] = jnp.dot(scaled, chosen_ref[...], preferred_element_type=f32) * (1.0 / cands**0.5)
        c = pltpu.make_async_copy(held.at[s], update_ref.at[s], sem.at[k])
        c.start()
        copies.append(c)
    for c in copies:
        c.wait()


def update_of(parts, counts, columns, chosen):
    depth, cands = columns.shape
    width = chosen.shape[1]
    step = next(s for s in (128, 64, 32, 16, depth) if depth % s == 0)
    return pl.pallas_call(
        functools.partial(update_kernel, step),
        in_specs=[vmem()] * 4,
        out_specs=[hbm(), vmem()],
        out_shape=[jax.ShapeDtypeStruct((depth, width), f32), jax.ShapeDtypeStruct((1, cands), f32)],
        scratch_shapes=[pltpu.VMEM((depth, width), f32), pltpu.SemaphoreType.DMA((depth // step,))],
        compiler_params=params(20),
        name="update",
    )(parts, counts, columns, chosen)


def hop(value, bit, devices):
    return lax.ppermute(value, AXES, [(i, i ^ bit) for i in range(devices)])


def place():
    grp = lax.axis_index("grp")
    return jnp.bitwise_and(grp, 1), jnp.bitwise_and(jnp.right_shift(grp, 1), 3)


def sent(heights, first, last):
    core, spot = place()
    early, late = heights
    near, far = 2 * spot + core, 2 * (3 - spot) + core
    base = PIECES * early
    return [near * early, base + near * late, far * early, base + far * late][first:last]


def arrived():
    core, spot = place()
    ids = [spot, jnp.bitwise_xor(spot, 1), jnp.bitwise_xor(spot, 2), 3 - spot]
    return [2 * i + core for i in ids] + [2 * i + 1 - core for i in ids]


def per_device(groups, parts, tokens, target, weight, factor_a, factor_b, counts, cand_index):
    return compute(groups, parts, tokens, target, weight, factor_a, factor_b, counts, cand_index)


def compute(groups, parts, tokens, target, weight, factor_a, factor_b, counts, cand_index):
    devices = groups * parts
    rows, full = tokens.shape
    depth = weight.shape[0]
    cands = counts.shape[0]
    noise = 0.5 * full ** (-0.5)
    index = cand_index.T
    if parts == 2 and groups % 8 == 0 and depth % (2 * PIECES * 16) == 0 and depth > 32 * PIECES:
        late = (depth // PIECES - SKEW) // 2
        heights = (depth // PIECES - late, late)
        (first,) = pack(functools.partial(sent, heights, 0, 1), heights[:1], index, weight, factor_a)
        second, third, fourth = pack(
            functools.partial(sent, heights, 1, 4), heights[::-1] + heights[1:], index, weight, factor_a
        )
        y1, y2 = hop(first, 1, devices), hop(second, 1, devices)
        y3, y4 = hop(third, 1, devices), hop(fourth, 1, devices)
        x1, z1 = hop(y1, 4, devices), hop(y1, 8, devices)
        x2, z2 = hop(y2, 4, devices), hop(y2, 8, devices)
        early, late = {"y1": y1, "x1": x1, "z1": z1, "y3": y3}, {"y2": y2, "x2": x2, "z2": z2, "y4": y4}
        early, late = (
            [*some.values()] + [hop(v, 2, devices) for v in some.values()] for some in (early, late)
        )
        far, base, sc, hot, right_rows, columns, chosen = near_half(
            index, counts[None, :], tokens, weight, factor_a, factor_b, target
        )
        base, sc = middle(arrived, far, base, sc, early)
        sums = losses(noise, arrived, far, base, sc, right_rows, hot, late, devices)
    else:
        left, right = cand_index[:, 0], cand_index[:, 1]
        cand_ids = jnp.arange(cands, dtype=jnp.int32)
        ends = jnp.sum(jnp.where(cand_ids[:, None] <= cand_ids[None, :], counts[:, None], 0), axis=0)
        position = lax.axis_index(AXES) * rows + jnp.arange(rows, dtype=jnp.int32)
        hot = (position[:, None] >= (ends - counts)[None, :]) & (position[:, None] < ends[None, :])
        owned = hot.astype(f32)
        columns = jnp.take(factor_a, left, axis=1)
        chosen = jnp.take(factor_b, right, axis=0)
        right_rows = jnp.dot(hot.astype(bf16), chosen, preferred_element_type=f32)
        all_weight = lax.all_gather(weight, "fsdp", axis=0, tiled=True)
        all_columns = lax.all_gather(columns, "fsdp", axis=0, tiled=True)
        base = jnp.dot(tokens, all_weight, preferred_element_type=f32)
        sc = jnp.dot(tokens, all_columns, preferred_element_type=f32)
        picked = noise * jnp.sum(owned * sc, axis=1)
        diff = base + picked[:, None] * right_rows - target.astype(f32)
        loss = jnp.mean(diff * diff, axis=1)
        sums = jnp.broadcast_to(jnp.sum(owned * loss[:, None], axis=0)[None, None, :], (devices, 1, cands))
    spread = lax.all_to_all(sums, AXES, split_axis=0, concat_axis=0, tiled=True)
    update, scores = update_of(spread, counts[None, :], columns, chosen)
    return update, scores[0]


def solution(mesh):
    in_specs = (
        P(AXES, None),
        P(AXES, None),
        P("fsdp", None),
        P("fsdp", None),
        P(),
        P(),
        P(),
    )
    return jax.shard_map(
        functools.partial(per_device, mesh.shape["grp"], mesh.shape["fsdp"]),
        mesh=mesh,
        in_specs=in_specs,
        out_specs=(P("fsdp", None), P()),
        check_vma=False,
    )
```

```python
import functools

import jax
import jax.numpy as jnp
from jax import lax
from jax.experimental import pallas as pl
from jax.experimental.pallas import tpu as pltpu
from jax.sharding import PartitionSpec as P


AXES = ("grp", "fsdp")
f32 = jnp.float32
bf16 = jnp.bfloat16
PIECES = 8
BATCH = 32


def turned(row, height):
    return jnp.transpose(jnp.broadcast_to(row.astype(f32), (height, row.shape[1])))


def matches(row, pool):
    ids = lax.broadcasted_iota(jnp.int32, (pool, row.shape[1]), 0)
    return (ids == row).astype(f32).astype(bf16)


def pack_kernel(order, weight_ref, *refs):
    outs, sem = refs[:-1], refs[-1]
    copies = []
    for k, (out, block) in enumerate(zip(outs, order())):
        height = out.shape[0]
        rows = pl.ds(pl.multiple_of(block * height, 16), height)
        copies.append(pltpu.make_async_copy(weight_ref.at[rows], out, sem.at[k]))
    for c in copies:
        c.start()
    for c in copies:
        c.wait()


def ends_of(counts_ref):
    cands = counts_ref.shape[1]
    along = lax.broadcasted_iota(jnp.int32, (cands, cands), 0)
    across = lax.broadcasted_iota(jnp.int32, (cands, cands), 1)
    return jnp.sum(jnp.where(along <= across, turned(counts_ref[...], cands), 0.0), axis=0, keepdims=True)


def first_of(ends, device, rows):
    return jnp.sum(jnp.where(ends <= (device * rows).astype(f32), 1.0, 0.0), axis=1, keepdims=True)


def batch_columns(lefts, first, factor):
    cands, pool = lefts.shape[1], factor.shape[1]
    ids = lax.broadcasted_iota(jnp.int32, (BATCH, cands), 1).astype(f32)
    rows = lax.broadcasted_iota(jnp.int32, (BATCH, cands), 0).astype(f32)
    left = jnp.sum(jnp.where(ids == first + rows, lefts.astype(f32), 0.0), axis=1, keepdims=True)
    places = lax.broadcasted_iota(jnp.int32, (BATCH, pool), 1).astype(f32)
    selector = jnp.where(places == left, 1.0, 0.0).astype(bf16)
    return across_dot(selector, factor).astype(bf16)


def across_dot(a, b):
    return lax.dot_general(a, b, (((1,), (1,)), ((), ())), preferred_element_type=f32)


def offer_kernel(tokens, index_ref, counts_ref, factor_ref, *refs):
    out_ref, a, sem = refs[-3:]
    copy = pltpu.make_async_copy(factor_ref, a, sem)
    copy.start()
    partner = lax.axis_index("grp") * lax.axis_size("fsdp") + 1 - lax.axis_index("fsdp")
    first = first_of(ends_of(counts_ref), partner, tokens)
    if len(refs) > 3:
        first = first + (refs[0][0] * BATCH).astype(f32)
    copy.wait()
    out_ref[...] = batch_columns(index_ref[0:1, :], first, a[...])


def offer(tokens, index, counts, factor_a, *turn):
    return pl.pallas_call(
        functools.partial(offer_kernel, tokens),
        in_specs=[vmem(), vmem(), hbm()] + [pl.BlockSpec(memory_space=pltpu.SMEM)] * len(turn),
        out_specs=vmem(),
        out_shape=jax.ShapeDtypeStruct((BATCH, factor_a.shape[0]), bf16),
        scratch_shapes=[pltpu.VMEM(factor_a.shape, bf16), pltpu.SemaphoreType.DMA],
        compiler_params=params(8),
        name="offer",
    )(index, counts, *in_hbm(factor_a), *turn)


def owners(ends, counts_ref, device, rows):
    begins = ends - counts_ref[...].astype(f32)
    position = (device * rows + lax.broadcasted_iota(jnp.int32, (rows, ends.shape[1]), 0)).astype(f32)
    return jnp.where((position >= begins) & (position < ends), 1.0, 0.0).astype(bf16)


def few_of(hot, first):
    ids = lax.broadcasted_iota(jnp.int32, (hot.shape[1], BATCH), 0).astype(f32)
    slots = lax.broadcasted_iota(jnp.int32, (hot.shape[1], BATCH), 1).astype(f32)
    return jnp.dot(hot, jnp.where(ids == first + slots, 1.0, 0.0).astype(bf16), preferred_element_type=f32)


def round_kernel(turn_ref, total_ref, cols_ref, index_ref, counts_ref, tokens_ref, factor_ref, out_ref, x, a, sem):
    fsdp = lax.axis_index("fsdp")
    device = lax.axis_index("grp") * lax.axis_size("fsdp") + fsdp
    rows, depth = x.shape[0], a.shape[0]
    copies = [pltpu.make_async_copy(tokens_ref, x, sem.at[0]), pltpu.make_async_copy(factor_ref, a, sem.at[1])]
    for c in copies:
        c.start()
    ends = ends_of(counts_ref)
    first = first_of(ends, device, rows) + (turn_ref[0] * BATCH).astype(f32)
    few = few_of(owners(ends, counts_ref, device, rows), first)
    for c in copies:
        c.wait()
    near = x[:, pl.ds(pl.multiple_of(fsdp * depth, 128), depth)]
    far = x[:, pl.ds(pl.multiple_of((1 - fsdp) * depth, 128), depth)]
    sc = across_dot(near, batch_columns(index_ref[0:1, :], first, a[...])) + across_dot(far, cols_ref[...])
    out_ref[...] = total_ref[...] + jnp.sum(few * sc, axis=1, keepdims=True)


def one_round(turn, total, cols, index, counts, tokens, factor_a):
    return pl.pallas_call(
        round_kernel,
        in_specs=[pl.BlockSpec(memory_space=pltpu.SMEM)] + [vmem()] * 4 + [hbm()] * 2,
        out_specs=vmem(),
        out_shape=jax.ShapeDtypeStruct(total.shape, f32),
        scratch_shapes=[
            pltpu.VMEM(tokens.shape, bf16), pltpu.VMEM(factor_a.shape, bf16), pltpu.SemaphoreType.DMA((2,)),
        ],
        compiler_params=params(16),
        name="round",
    )(turn, total, cols, index, counts, *in_hbm(tokens, factor_a))


def vmem():
    return pl.BlockSpec(memory_space=pltpu.VMEM)


def hbm():
    return pl.BlockSpec(memory_space=pltpu.HBM)


def in_hbm(*arrays):
    return [pltpu.with_memory_space_constraint(a, pltpu.HBM) for a in arrays]


def params(mib):
    return pltpu.CompilerParams(vmem_limit_bytes=mib << 20)


def pack(order, heights, weight):
    width = weight.shape[1]
    return pl.pallas_call(
        functools.partial(pack_kernel, order),
        in_specs=[hbm()],
        out_specs=[vmem()] * len(heights),
        out_shape=[jax.ShapeDtypeStruct((h, width), bf16) for h in heights],
        scratch_shapes=[pltpu.SemaphoreType.DMA((len(heights),))],
        compiler_params=params(4),
        name="pack",
    )(*in_hbm(weight))


def near_kernel(tokens_ref, weight_ref, target_ref, near_ref, far_ref, base_ref, w, t, sem):
    fsdp = lax.axis_index("fsdp")
    depth = far_ref.shape[1]
    near = pl.ds(pl.multiple_of(fsdp * depth, 128), depth)
    other = pl.ds(pl.multiple_of((1 - fsdp) * depth, 128), depth)
    pairs = [
        (tokens_ref.at[:, near], near_ref), (weight_ref, w), (target_ref, t), (tokens_ref.at[:, other], far_ref),
    ]
    copies = [pltpu.make_async_copy(s, d, sem.at[k]) for k, (s, d) in enumerate(pairs)]
    for c in copies:
        c.start()
    for c in copies[:3]:
        c.wait()
    base_ref[...] = jnp.dot(near_ref[...], w[...], preferred_element_type=f32) - t[...].astype(f32)
    copies[3].wait()


def near_half(tokens, weight, target):
    rows, width = target.shape
    depth = weight.shape[0]
    return pl.pallas_call(
        near_kernel,
        in_specs=[hbm()] * 3,
        out_specs=[vmem()] * 3,
        out_shape=[
            jax.ShapeDtypeStruct((rows, depth), bf16), jax.ShapeDtypeStruct((rows, depth), bf16),
            jax.ShapeDtypeStruct((rows, width), f32),
        ],
        scratch_shapes=[
            pltpu.VMEM((depth, width), bf16), pltpu.VMEM((rows, width), bf16), pltpu.SemaphoreType.DMA((4,)),
        ],
        compiler_params=params(14),
        cost_estimate=pl.CostEstimate(flops=8 * rows * depth * width, bytes_accessed=8 << 20, transcendentals=0),
        name="near",
    )(*in_hbm(tokens, weight, target))


def tables_kernel(
    index_ref, counts_ref, near_ref, factor_ref, rights_ref,
    sc_ref, hot_ref, few_ref, right_ref, columns_ref, chosen_ref, a, b, sem,
):
    device = lax.axis_index("grp") * lax.axis_size("fsdp") + lax.axis_index("fsdp")
    rows, pool = near_ref.shape[0], factor_ref.shape[1]
    copies = [pltpu.make_async_copy(s, d, sem.at[k]) for k, (s, d) in enumerate([(rights_ref, b), (factor_ref, a)])]
    for c in copies:
        c.start()
    ends = ends_of(counts_ref)
    first = first_of(ends, device, rows)
    hot = owners(ends, counts_ref, device, rows)
    hot_ref[...] = hot
    few_ref[...] = few_of(hot, first)
    copies[0].wait()
    chosen = lax.dot_general(
        matches(index_ref[1:2, :], pool), b[...], (((0,), (0,)), ((), ())), preferred_element_type=f32
    ).astype(bf16)
    chosen_ref[...] = chosen
    right_ref[...] = jnp.dot(hot, chosen, preferred_element_type=f32).astype(bf16)
    copies[1].wait()
    columns_ref[...] = jnp.dot(a[...], matches(index_ref[0:1, :], pool), preferred_element_type=f32).astype(bf16)
    sc_ref[...] = across_dot(near_ref[...], batch_columns(index_ref[0:1, :], first, a[...]))


def tables(index, counts, near, factor_a, factor_b):
    rows, depth = near.shape
    (pool, width), cands = factor_b.shape, counts.shape[1]

    def shaped(*shape, dtype=bf16):
        return jax.ShapeDtypeStruct(shape, dtype)

    return pl.pallas_call(
        tables_kernel,
        in_specs=[vmem()] * 3 + [hbm()] * 2,
        out_specs=[vmem()] * 6,
        out_shape=[
            shaped(rows, BATCH, dtype=f32), shaped(rows, cands), shaped(rows, BATCH, dtype=f32),
            shaped(rows, width), shaped(depth, cands), shaped(cands, width),
        ],
        scratch_shapes=[
            pltpu.VMEM((depth, pool), bf16), pltpu.VMEM((pool, width), bf16), pltpu.SemaphoreType.DMA((2,)),
        ],
        compiler_params=params(12),
        cost_estimate=pl.CostEstimate(flops=8 * rows * depth * width, bytes_accessed=4 << 20, transcendentals=0),
        name="tables",
    )(index, counts, near, *in_hbm(factor_a, factor_b))


def stack(pieces, blocks, held):
    height = pieces[0].shape[0]
    for piece, block in zip(pieces, blocks):
        held[pl.ds(pl.multiple_of(block * height, 16), height), :] = piece[...]


def middle_kernel(order, x_ref, base_ref, sc_ref, cols_ref, *refs):
    pieces, base_out, sc_out, held = refs[:-3], *refs[-3:]
    stack(pieces, order(), held)
    rows = base_ref.shape[0]
    half = held.shape[0]
    step = 128
    for r in range(0, rows, step):
        s = slice(r, r + step)
        acc = jnp.dot(x_ref[s, :half], held[...], preferred_element_type=f32)
        base_out[s, :] = base_ref[s, :] + acc
        sc_out[s, :] = sc_ref[s, :] + across_dot(x_ref[s, :], cols_ref[...])


def middle(order, x, base, sc, cols, pieces):
    depth, columns = x.shape[1], base.shape[1]
    return pl.pallas_call(
        functools.partial(middle_kernel, order),
        in_specs=[vmem()] * (4 + len(pieces)),
        out_specs=[vmem()] * 2,
        out_shape=[jax.ShapeDtypeStruct(base.shape, f32), jax.ShapeDtypeStruct(sc.shape, f32)],
        scratch_shapes=[pltpu.VMEM((sum(p.shape[0] for p in pieces), columns), bf16)],
        compiler_params=params(12),
        cost_estimate=pl.CostEstimate(
            flops=4 * x.shape[0] * depth * columns, bytes_accessed=4 << 20, transcendentals=0
        ),
        name="middle",
    )(x, base, sc, cols, *pieces)


def loss_kernel(noise, order, x_ref, base_ref, sc_ref, few_ref, more_ref, right_ref, hot_ref, *refs):
    pieces, out_ref, held = refs[:-2], refs[-2], refs[-1]
    stack(pieces, order(), held)
    rows, width = base_ref.shape
    half = held.shape[0]
    total = None
    step = 128
    for r in range(0, rows, step):
        s = slice(r, r + step)
        acc = jnp.dot(x_ref[s, x_ref.shape[1] - half :], held[...], preferred_element_type=f32)
        hot = hot_ref[s, :].astype(f32)
        picked = (jnp.sum(few_ref[s, :] * sc_ref[s, :], axis=1, keepdims=True) + more_ref[s, :]) * noise
        diff = acc + base_ref[s, :] + picked * right_ref[s, :].astype(f32)
        loss = jnp.sum(diff * diff, axis=1, keepdims=True) * (1.0 / width)
        part = jnp.sum(hot * loss, axis=0, keepdims=True)
        total = part if total is None else total + part
    out_ref[...] = jnp.broadcast_to(total[None], out_ref.shape)


def losses(noise, order, x, base, sc, few, more, right, hot, pieces, devices):
    width, cands = base.shape[1], hot.shape[1]
    return pl.pallas_call(
        functools.partial(loss_kernel, noise, order),
        in_specs=[vmem()] * (7 + len(pieces)),
        out_specs=vmem(),
        out_shape=jax.ShapeDtypeStruct((devices, 1, cands), f32),
        scratch_shapes=[pltpu.VMEM((sum(p.shape[0] for p in pieces), width), bf16)],
        compiler_params=params(12),
        name="losses",
    )(x, base, sc, few, more, right, hot, *pieces)


def update_kernel(step, parts_ref, counts_ref, columns_ref, chosen_ref, update_ref, scores_ref, held, sem):
    cands = counts_ref.shape[1]
    totals = jnp.sum(parts_ref[...], axis=0)
    fitness = -totals / counts_ref[...].astype(f32)
    middle = jnp.sum(fitness, axis=1, keepdims=True) / cands
    spread = jnp.sum((fitness - middle) ** 2, axis=1, keepdims=True) / cands
    scores = (fitness - middle) / jnp.sqrt(spread + 1e-06)
    scores_ref[...] = scores
    copies = []
    for k in range(columns_ref.shape[0] // step):
        s = pl.ds(k * step, step)
        scaled = (columns_ref[s, :].astype(f32) * scores).astype(bf16)
        held[s, :] = jnp.dot(scaled, chosen_ref[...], preferred_element_type=f32) * (1.0 / cands**0.5)
        c = pltpu.make_async_copy(held.at[s], update_ref.at[s], sem.at[k])
        c.start()
        copies.append(c)
    for c in copies:
        c.wait()


def update_of(parts, counts, columns, chosen):
    depth, cands = columns.shape
    width = chosen.shape[1]
    step = next(s for s in (128, 64, 32, 16, depth) if depth % s == 0)
    return pl.pallas_call(
        functools.partial(update_kernel, step),
        in_specs=[vmem()] * 4,
        out_specs=[hbm(), vmem()],
        out_shape=[jax.ShapeDtypeStruct((depth, width), f32), jax.ShapeDtypeStruct((1, cands), f32)],
        scratch_shapes=[pltpu.VMEM((depth, width), f32), pltpu.SemaphoreType.DMA((depth // step,))],
        compiler_params=params(12),
        name="update",
    )(parts, counts, columns, chosen)


def hop(value, bit, devices):
    return lax.ppermute(value, AXES, [(i, i ^ bit) for i in range(devices)])


def place():
    grp = lax.axis_index("grp")
    return jnp.bitwise_and(grp, 1), jnp.bitwise_and(jnp.right_shift(grp, 1), 3)


def sent():
    core, spot = place()
    return [2 * i + core for i in (spot, spot + 4, 3 - spot, 7 - spot)]


def further(rounds, index, counts, tokens, factor_a):
    rows, devices = tokens.shape[0], lax.axis_size("grp") * lax.axis_size("fsdp")

    def one(k, total):
        turn = jnp.full((1,), k, jnp.int32)
        theirs = hop(offer(rows, index, counts, factor_a, turn), 1, devices)
        return one_round(turn, total, theirs, index, counts, tokens, factor_a)

    return lax.fori_loop(1, rounds, one, jnp.zeros((rows, 1), f32))


def rounds_of(counts, rows, devices):
    ids = jnp.arange(counts.shape[0], dtype=jnp.int32)
    ends = jnp.sum(jnp.where(ids[:, None] <= ids[None, :], counts[:, None], 0), axis=0)
    starts = jnp.arange(devices, dtype=jnp.int32)[:, None] * rows
    inside = (ends[None, :] > starts) & ((ends - counts)[None, :] < starts + rows)
    most = jnp.max(jnp.sum(inside.astype(jnp.int32), axis=1))
    return (most + BATCH - 1) // BATCH


def arrived():
    core, spot = place()
    ids = [spot, jnp.bitwise_xor(spot, 1), jnp.bitwise_xor(spot, 2), 3 - spot]
    return [2 * i + core for i in ids] + [2 * i + 1 - core for i in ids]


def per_device(groups, parts, tokens, target, weight, factor_a, factor_b, counts, cand_index):
    return compute(groups, parts, tokens, target, weight, factor_a, factor_b, counts, cand_index)


def compute(groups, parts, tokens, target, weight, factor_a, factor_b, counts, cand_index):
    devices = groups * parts
    rows, full = tokens.shape
    depth = weight.shape[0]
    cands = counts.shape[0]
    noise = 0.5 * full ** (-0.5)
    index = cand_index.T
    if parts == 2 and groups % 8 == 0 and depth % (2 * PIECES * 16) == 0:
        height = depth // (2 * PIECES)
        first, second, third, fourth = pack(sent, [height] * 4, weight)
        given = offer(rows, index, counts[None, :], factor_a)
        more = further(rounds_of(counts, rows, devices), index, counts[None, :], tokens, factor_a)
        y1, y2 = hop(first, 1, devices), hop(second, 1, devices)
        y3, y4 = hop(third, 1, devices), hop(fourth, 1, devices)
        taken = hop(given, 1, devices)
        x1, z1 = hop(y1, 4, devices), hop(y1, 8, devices)
        x2, z2 = hop(y2, 4, devices), hop(y2, 8, devices)
        early, late = {"y1": y1, "x1": x1, "z1": z1, "y3": y3}, {"y2": y2, "x2": x2, "z2": z2, "y4": y4}
        early, late = (
            [*some.values()] + [hop(v, 2, devices) for v in some.values()] for some in (early, late)
        )
        near, far, base = near_half(tokens, weight, target)
        sc, hot, few, right_rows, columns, chosen = tables(index, counts[None, :], near, factor_a, factor_b)
        base, sc = middle(arrived, far, base, sc, taken, early)
        sums = losses(noise, arrived, far, base, sc, few, more, right_rows, hot, late, devices)
    else:
        left, right = cand_index[:, 0], cand_index[:, 1]
        cand_ids = jnp.arange(cands, dtype=jnp.int32)
        ends = jnp.sum(jnp.where(cand_ids[:, None] <= cand_ids[None, :], counts[:, None], 0), axis=0)
        position = lax.axis_index(AXES) * rows + jnp.arange(rows, dtype=jnp.int32)
        hot = (position[:, None] >= (ends - counts)[None, :]) & (position[:, None] < ends[None, :])
        owned = hot.astype(f32)
        columns = jnp.take(factor_a, left, axis=1)
        chosen = jnp.take(factor_b, right, axis=0)
        right_rows = jnp.dot(hot.astype(bf16), chosen, preferred_element_type=f32)
        all_weight = lax.all_gather(weight, "fsdp", axis=0, tiled=True)
        all_columns = lax.all_gather(columns, "fsdp", axis=0, tiled=True)
        base = jnp.dot(tokens, all_weight, preferred_element_type=f32)
        sc = jnp.dot(tokens, all_columns, preferred_element_type=f32)
        picked = noise * jnp.sum(owned * sc, axis=1)
        diff = base + picked[:, None] * right_rows - target.astype(f32)
        loss = jnp.mean(diff * diff, axis=1)
        sums = jnp.broadcast_to(jnp.sum(owned * loss[:, None], axis=0)[None, None, :], (devices, 1, cands))
    spread = lax.all_to_all(sums, AXES, split_axis=0, concat_axis=0, tiled=True)
    update, scores = update_of(spread, counts[None, :], columns, chosen)
    return update, scores[0]


def solution(mesh):
    in_specs = (
        P(AXES, None),
        P(AXES, None),
        P("fsdp", None),
        P("fsdp", None),
        P(),
        P(),
        P(),
    )
    return jax.shard_map(
        functools.partial(per_device, mesh.shape["grp"], mesh.shape["fsdp"]),
        mesh=mesh,
        in_specs=in_specs,
        out_specs=(P("fsdp", None), P()),
        check_vma=False,
    )
```

```python
import functools

import jax
import jax.numpy as jnp
from jax import lax
from jax.experimental import pallas as pl
from jax.experimental.pallas import tpu as pltpu
from jax.sharding import PartitionSpec as P


AXES = ("grp", "fsdp")
f32 = jnp.float32
bf16 = jnp.bfloat16
PIECES = 8
BATCH = 32
CUT = 640


def turned(row, height):
    return jnp.transpose(jnp.broadcast_to(row.astype(f32), (height, row.shape[1])))


def matches(row, pool):
    ids = lax.broadcasted_iota(jnp.int32, (pool, row.shape[1]), 0)
    return (ids == row).astype(f32).astype(bf16)


def pack_kernel(order, weight_ref, *refs):
    outs, sem = refs[:-1], refs[-1]
    copies = []
    for k, (out, block) in enumerate(zip(outs, order())):
        height = out.shape[0]
        rows = pl.ds(pl.multiple_of(block * height, 16), height)
        copies.append(pltpu.make_async_copy(weight_ref.at[rows], out, sem.at[k]))
    for c in copies:
        c.start()
    for c in copies:
        c.wait()


def ends_of(counts_ref):
    cands = counts_ref.shape[1]
    along = lax.broadcasted_iota(jnp.int32, (cands, cands), 0)
    across = lax.broadcasted_iota(jnp.int32, (cands, cands), 1)
    return jnp.sum(jnp.where(along <= across, turned(counts_ref[...], cands), 0.0), axis=0, keepdims=True)


def first_of(ends, device, rows):
    return jnp.sum(jnp.where(ends <= (device * rows).astype(f32), 1.0, 0.0), axis=1, keepdims=True)


def batch_columns(lefts, first, factor):
    cands, pool = lefts.shape[1], factor.shape[1]
    ids = lax.broadcasted_iota(jnp.int32, (BATCH, cands), 1).astype(f32)
    rows = lax.broadcasted_iota(jnp.int32, (BATCH, cands), 0).astype(f32)
    left = jnp.sum(jnp.where(ids == first + rows, lefts.astype(f32), 0.0), axis=1, keepdims=True)
    places = lax.broadcasted_iota(jnp.int32, (BATCH, pool), 1).astype(f32)
    selector = jnp.where(places == left, 1.0, 0.0).astype(bf16)
    return across_dot(selector, factor).astype(bf16)


def across_dot(a, b):
    return lax.dot_general(a, b, (((1,), (1,)), ((), ())), preferred_element_type=f32)


def offer_kernel(tokens, index_ref, counts_ref, factor_ref, *refs):
    out_ref, a, sem = refs[-3:]
    copy = pltpu.make_async_copy(factor_ref, a, sem)
    copy.start()
    partner = lax.axis_index("grp") * lax.axis_size("fsdp") + 1 - lax.axis_index("fsdp")
    first = first_of(ends_of(counts_ref), partner, tokens)
    if len(refs) > 3:
        first = first + (refs[0][0] * BATCH).astype(f32)
    copy.wait()
    out_ref[...] = batch_columns(index_ref[0:1, :], first, a[...])


def offer(tokens, index, counts, factor_a, *turn):
    return pl.pallas_call(
        functools.partial(offer_kernel, tokens),
        in_specs=[vmem(), vmem(), hbm()] + [pl.BlockSpec(memory_space=pltpu.SMEM)] * len(turn),
        out_specs=vmem(),
        out_shape=jax.ShapeDtypeStruct((BATCH, factor_a.shape[0]), bf16),
        scratch_shapes=[pltpu.VMEM(factor_a.shape, bf16), pltpu.SemaphoreType.DMA],
        compiler_params=params(8),
        name="offer",
    )(index, counts, *in_hbm(factor_a), *turn)


def owners(ends, counts_ref, device, rows):
    begins = ends - counts_ref[...].astype(f32)
    position = (device * rows + lax.broadcasted_iota(jnp.int32, (rows, ends.shape[1]), 0)).astype(f32)
    return jnp.where((position >= begins) & (position < ends), 1.0, 0.0).astype(bf16)


def few_of(hot, first):
    ids = lax.broadcasted_iota(jnp.int32, (hot.shape[1], BATCH), 0).astype(f32)
    slots = lax.broadcasted_iota(jnp.int32, (hot.shape[1], BATCH), 1).astype(f32)
    return jnp.dot(hot, jnp.where(ids == first + slots, 1.0, 0.0).astype(bf16), preferred_element_type=f32)


def round_kernel(turn_ref, total_ref, cols_ref, index_ref, counts_ref, tokens_ref, factor_ref, out_ref, x, a, sem):
    fsdp = lax.axis_index("fsdp")
    device = lax.axis_index("grp") * lax.axis_size("fsdp") + fsdp
    rows, depth = x.shape[0], a.shape[0]
    copies = [pltpu.make_async_copy(tokens_ref, x, sem.at[0]), pltpu.make_async_copy(factor_ref, a, sem.at[1])]
    for c in copies:
        c.start()
    ends = ends_of(counts_ref)
    first = first_of(ends, device, rows) + (turn_ref[0] * BATCH).astype(f32)
    few = few_of(owners(ends, counts_ref, device, rows), first)
    for c in copies:
        c.wait()
    near = x[:, pl.ds(pl.multiple_of(fsdp * depth, 128), depth)]
    far = x[:, pl.ds(pl.multiple_of((1 - fsdp) * depth, 128), depth)]
    sc = across_dot(near, batch_columns(index_ref[0:1, :], first, a[...])) + across_dot(far, cols_ref[...])
    out_ref[...] = total_ref[...] + jnp.sum(few * sc, axis=1, keepdims=True)


def one_round(turn, total, cols, index, counts, tokens, factor_a):
    return pl.pallas_call(
        round_kernel,
        in_specs=[pl.BlockSpec(memory_space=pltpu.SMEM)] + [vmem()] * 4 + [hbm()] * 2,
        out_specs=vmem(),
        out_shape=jax.ShapeDtypeStruct(total.shape, f32),
        scratch_shapes=[
            pltpu.VMEM(tokens.shape, bf16), pltpu.VMEM(factor_a.shape, bf16), pltpu.SemaphoreType.DMA((2,)),
        ],
        compiler_params=params(16),
        name="round",
    )(turn, total, cols, index, counts, *in_hbm(tokens, factor_a))


def vmem():
    return pl.BlockSpec(memory_space=pltpu.VMEM)


def hbm():
    return pl.BlockSpec(memory_space=pltpu.HBM)


def in_hbm(*arrays):
    return [pltpu.with_memory_space_constraint(a, pltpu.HBM) for a in arrays]


def params(mib):
    return pltpu.CompilerParams(vmem_limit_bytes=mib << 20)


def pack(order, heights, weight):
    width = weight.shape[1]
    return pl.pallas_call(
        functools.partial(pack_kernel, order),
        in_specs=[hbm()],
        out_specs=[vmem()] * len(heights),
        out_shape=[jax.ShapeDtypeStruct((h, width), bf16) for h in heights],
        scratch_shapes=[pltpu.SemaphoreType.DMA((len(heights),))],
        compiler_params=params(4),
        name="pack",
    )(*in_hbm(weight))


def near_kernel(
    tokens_ref, weight_ref, target_ref, factor_ref, rights_ref, near_ref, far_ref, base_ref, a_ref, b_ref, w, t, sem
):
    fsdp = lax.axis_index("fsdp")
    depth = far_ref.shape[1]
    near = pl.ds(pl.multiple_of(fsdp * depth, 128), depth)
    other = pl.ds(pl.multiple_of((1 - fsdp) * depth, 128), depth)
    cuts = [pl.ds(k, min(CUT, depth - k)) for k in range(0, depth, CUT)]
    pairs = [(tokens_ref.at[:, near], near_ref)] + [(weight_ref.at[cut], w.at[cut]) for cut in cuts]
    pairs += [(target_ref, t), (rights_ref, b_ref), (factor_ref, a_ref), (tokens_ref.at[:, other], far_ref)]
    copies = [pltpu.make_async_copy(s, d, sem.at[k]) for k, (s, d) in enumerate(pairs)]
    for c in copies:
        c.start()
    copies[0].wait()
    for k, cut in enumerate(cuts):
        copies[1 + k].wait()
        part = jnp.dot(near_ref[:, cut], w[cut, :], preferred_element_type=f32)
        if k + 1 == len(cuts):
            copies[-4].wait()
            part = part - t[...].astype(f32)
        base_ref[...] = part if k == 0 else base_ref[...] + part
    for c in copies[-3:]:
        c.wait()


def near_half(tokens, weight, target, factor_a, factor_b):
    rows, width = target.shape
    depth = weight.shape[0]
    return pl.pallas_call(
        near_kernel,
        in_specs=[hbm()] * 5,
        out_specs=[vmem()] * 5,
        out_shape=[
            jax.ShapeDtypeStruct((rows, depth), bf16), jax.ShapeDtypeStruct((rows, depth), bf16),
            jax.ShapeDtypeStruct((rows, width), f32), jax.ShapeDtypeStruct(factor_a.shape, bf16),
            jax.ShapeDtypeStruct(factor_b.shape, bf16),
        ],
        scratch_shapes=[
            pltpu.VMEM((depth, width), bf16), pltpu.VMEM((rows, width), bf16),
            pltpu.SemaphoreType.DMA((5 + -(-depth // CUT),)),
        ],
        compiler_params=params(14),
        cost_estimate=pl.CostEstimate(flops=8 * rows * depth * width, bytes_accessed=8 << 20, transcendentals=0),
        name="near",
    )(*in_hbm(tokens, weight, target, factor_a, factor_b))


def tables_kernel(
    index_ref, counts_ref, near_ref, a, b, sc_ref, hot_ref, few_ref, right_ref, columns_ref, chosen_ref
):
    device = lax.axis_index("grp") * lax.axis_size("fsdp") + lax.axis_index("fsdp")
    rows, pool = near_ref.shape[0], a.shape[1]
    ends = ends_of(counts_ref)
    first = first_of(ends, device, rows)
    hot = owners(ends, counts_ref, device, rows)
    hot_ref[...] = hot
    few_ref[...] = few_of(hot, first)
    chosen = lax.dot_general(
        matches(index_ref[1:2, :], pool), b[...], (((0,), (0,)), ((), ())), preferred_element_type=f32
    ).astype(bf16)
    chosen_ref[...] = chosen
    right_ref[...] = jnp.dot(hot, chosen, preferred_element_type=f32).astype(bf16)
    columns_ref[...] = jnp.dot(a[...], matches(index_ref[0:1, :], pool), preferred_element_type=f32).astype(bf16)
    sc_ref[...] = across_dot(near_ref[...], batch_columns(index_ref[0:1, :], first, a[...]))


def tables(index, counts, near, factor_a, factor_b):
    rows, depth = near.shape
    width, cands = factor_b.shape[1], counts.shape[1]

    def shaped(*shape, dtype=bf16):
        return jax.ShapeDtypeStruct(shape, dtype)

    return pl.pallas_call(
        tables_kernel,
        in_specs=[vmem()] * 5,
        out_specs=[vmem()] * 6,
        out_shape=[
            shaped(rows, BATCH, dtype=f32), shaped(rows, cands), shaped(rows, BATCH, dtype=f32),
            shaped(rows, width), shaped(depth, cands), shaped(cands, width),
        ],
        compiler_params=params(12),
        cost_estimate=pl.CostEstimate(flops=8 * rows * depth * width, bytes_accessed=4 << 20, transcendentals=0),
        name="tables",
    )(index, counts, near, factor_a, factor_b)


def stack(pieces, blocks, held):
    height = pieces[0].shape[0]
    for piece, block in zip(pieces, blocks):
        held[pl.ds(pl.multiple_of(block * height, 16), height), :] = piece[...]


def middle_kernel(order, x_ref, base_ref, sc_ref, cols_ref, *refs):
    pieces, base_out, sc_out, held = refs[:-3], *refs[-3:]
    stack(pieces, order(), held)
    rows = base_ref.shape[0]
    half = held.shape[0]
    step = 128
    for r in range(0, rows, step):
        s = slice(r, r + step)
        acc = jnp.dot(x_ref[s, :half], held[...], preferred_element_type=f32)
        base_out[s, :] = base_ref[s, :] + acc
        sc_out[s, :] = sc_ref[s, :] + across_dot(x_ref[s, :], cols_ref[...])


def middle(order, x, base, sc, cols, pieces):
    depth, columns = x.shape[1], base.shape[1]
    return pl.pallas_call(
        functools.partial(middle_kernel, order),
        in_specs=[vmem()] * (4 + len(pieces)),
        out_specs=[vmem()] * 2,
        out_shape=[jax.ShapeDtypeStruct(base.shape, f32), jax.ShapeDtypeStruct(sc.shape, f32)],
        scratch_shapes=[pltpu.VMEM((sum(p.shape[0] for p in pieces), columns), bf16)],
        compiler_params=params(12),
        cost_estimate=pl.CostEstimate(
            flops=4 * x.shape[0] * depth * columns, bytes_accessed=4 << 20, transcendentals=0
        ),
        name="middle",
    )(x, base, sc, cols, *pieces)


def loss_kernel(noise, order, x_ref, base_ref, sc_ref, few_ref, more_ref, right_ref, hot_ref, *refs):
    pieces, out_ref, held = refs[:-2], refs[-2], refs[-1]
    stack(pieces, order(), held)
    rows, width = base_ref.shape
    half = held.shape[0]
    total = None
    step = 128
    for r in range(0, rows, step):
        s = slice(r, r + step)
        acc = jnp.dot(x_ref[s, x_ref.shape[1] - half :], held[...], preferred_element_type=f32)
        hot = hot_ref[s, :].astype(f32)
        picked = (jnp.sum(few_ref[s, :] * sc_ref[s, :], axis=1, keepdims=True) + more_ref[s, :]) * noise
        diff = acc + base_ref[s, :] + picked * right_ref[s, :].astype(f32)
        loss = jnp.sum(diff * diff, axis=1, keepdims=True) * (1.0 / width)
        part = jnp.sum(hot * loss, axis=0, keepdims=True)
        total = part if total is None else total + part
    out_ref[...] = jnp.broadcast_to(total[None], out_ref.shape)


def losses(noise, order, x, base, sc, few, more, right, hot, pieces, devices):
    width, cands = base.shape[1], hot.shape[1]
    return pl.pallas_call(
        functools.partial(loss_kernel, noise, order),
        in_specs=[vmem()] * (7 + len(pieces)),
        out_specs=vmem(),
        out_shape=jax.ShapeDtypeStruct((devices, 1, cands), f32),
        scratch_shapes=[pltpu.VMEM((sum(p.shape[0] for p in pieces), width), bf16)],
        compiler_params=params(12),
        name="losses",
    )(x, base, sc, few, more, right, hot, *pieces)


def update_kernel(step, parts_ref, counts_ref, columns_ref, chosen_ref, update_ref, scores_ref, held, sem):
    cands = counts_ref.shape[1]
    totals = jnp.sum(parts_ref[...], axis=0)
    fitness = -totals / counts_ref[...].astype(f32)
    middle = jnp.sum(fitness, axis=1, keepdims=True) / cands
    spread = jnp.sum((fitness - middle) ** 2, axis=1, keepdims=True) / cands
    scores = (fitness - middle) / jnp.sqrt(spread + 1e-06)
    scores_ref[...] = scores
    copies = []
    for k in range(columns_ref.shape[0] // step):
        s = pl.ds(k * step, step)
        scaled = (columns_ref[s, :].astype(f32) * scores).astype(bf16)
        held[s, :] = jnp.dot(scaled, chosen_ref[...], preferred_element_type=f32) * (1.0 / cands**0.5)
        c = pltpu.make_async_copy(held.at[s], update_ref.at[s], sem.at[k])
        c.start()
        copies.append(c)
    for c in copies:
        c.wait()


def update_of(parts, counts, columns, chosen):
    depth, cands = columns.shape
    width = chosen.shape[1]
    step = next(s for s in (128, 64, 32, 16, depth) if depth % s == 0)
    return pl.pallas_call(
        functools.partial(update_kernel, step),
        in_specs=[vmem()] * 4,
        out_specs=[hbm(), vmem()],
        out_shape=[jax.ShapeDtypeStruct((depth, width), f32), jax.ShapeDtypeStruct((1, cands), f32)],
        scratch_shapes=[pltpu.VMEM((depth, width), f32), pltpu.SemaphoreType.DMA((depth // step,))],
        compiler_params=params(12),
        name="update",
    )(parts, counts, columns, chosen)


def hop(value, bit, devices):
    return lax.ppermute(value, AXES, [(i, i ^ bit) for i in range(devices)])


def place():
    grp = lax.axis_index("grp")
    return jnp.bitwise_and(grp, 1), jnp.bitwise_and(jnp.right_shift(grp, 1), 3)


def sent():
    core, spot = place()
    return [2 * i + core for i in (spot, spot + 4, 3 - spot, 7 - spot)]


def further(rounds, index, counts, tokens, factor_a):
    rows, devices = tokens.shape[0], lax.axis_size("grp") * lax.axis_size("fsdp")

    def one(k, total):
        turn = jnp.full((1,), k, jnp.int32)
        theirs = hop(offer(rows, index, counts, factor_a, turn), 1, devices)
        return one_round(turn, total, theirs, index, counts, tokens, factor_a)

    return lax.fori_loop(1, rounds, one, jnp.zeros((rows, 1), f32))


def rounds_of(counts, rows, devices):
    ids = jnp.arange(counts.shape[0], dtype=jnp.int32)
    ends = jnp.sum(jnp.where(ids[:, None] <= ids[None, :], counts[:, None], 0), axis=0)
    starts = jnp.arange(devices, dtype=jnp.int32)[:, None] * rows
    inside = (ends[None, :] > starts) & ((ends - counts)[None, :] < starts + rows)
    most = jnp.max(jnp.sum(inside.astype(jnp.int32), axis=1))
    return (most + BATCH - 1) // BATCH


def arrived():
    core, spot = place()
    ids = [spot, jnp.bitwise_xor(spot, 1), jnp.bitwise_xor(spot, 2), 3 - spot]
    return [2 * i + core for i in ids] + [2 * i + 1 - core for i in ids]


def per_device(groups, parts, tokens, target, weight, factor_a, factor_b, counts, cand_index):
    return compute(groups, parts, tokens, target, weight, factor_a, factor_b, counts, cand_index)


def compute(groups, parts, tokens, target, weight, factor_a, factor_b, counts, cand_index):
    devices = groups * parts
    rows, full = tokens.shape
    depth = weight.shape[0]
    cands = counts.shape[0]
    noise = 0.5 * full ** (-0.5)
    index = cand_index.T
    if parts == 2 and groups % 8 == 0 and depth % (2 * PIECES * 16) == 0:
        height = depth // (2 * PIECES)
        first, second, third, fourth = pack(sent, [height] * 4, weight)
        given = offer(rows, index, counts[None, :], factor_a)
        more = further(rounds_of(counts, rows, devices), index, counts[None, :], tokens, factor_a)
        y1, y2 = hop(first, 1, devices), hop(second, 1, devices)
        y3, y4 = hop(third, 1, devices), hop(fourth, 1, devices)
        taken = hop(given, 1, devices)
        x1, z1 = hop(y1, 4, devices), hop(y1, 8, devices)
        x2, z2 = hop(y2, 4, devices), hop(y2, 8, devices)
        early, late = {"y1": y1, "x1": x1, "z1": z1, "y3": y3}, {"y2": y2, "x2": x2, "z2": z2, "y4": y4}
        early, late = (
            [*some.values()] + [hop(v, 2, devices) for v in some.values()] for some in (early, late)
        )
        near, far, base, held_a, held_b = near_half(tokens, weight, target, factor_a, factor_b)
        sc, hot, few, right_rows, columns, chosen = tables(index, counts[None, :], near, held_a, held_b)
        base, sc = middle(arrived, far, base, sc, taken, early)
        sums = losses(noise, arrived, far, base, sc, few, more, right_rows, hot, late, devices)
    else:
        left, right = cand_index[:, 0], cand_index[:, 1]
        cand_ids = jnp.arange(cands, dtype=jnp.int32)
        ends = jnp.sum(jnp.where(cand_ids[:, None] <= cand_ids[None, :], counts[:, None], 0), axis=0)
        position = lax.axis_index(AXES) * rows + jnp.arange(rows, dtype=jnp.int32)
        hot = (position[:, None] >= (ends - counts)[None, :]) & (position[:, None] < ends[None, :])
        owned = hot.astype(f32)
        columns = jnp.take(factor_a, left, axis=1)
        chosen = jnp.take(factor_b, right, axis=0)
        right_rows = jnp.dot(hot.astype(bf16), chosen, preferred_element_type=f32)
        all_weight = lax.all_gather(weight, "fsdp", axis=0, tiled=True)
        all_columns = lax.all_gather(columns, "fsdp", axis=0, tiled=True)
        base = jnp.dot(tokens, all_weight, preferred_element_type=f32)
        sc = jnp.dot(tokens, all_columns, preferred_element_type=f32)
        picked = noise * jnp.sum(owned * sc, axis=1)
        diff = base + picked[:, None] * right_rows - target.astype(f32)
        loss = jnp.mean(diff * diff, axis=1)
        sums = jnp.broadcast_to(jnp.sum(owned * loss[:, None], axis=0)[None, None, :], (devices, 1, cands))
    spread = lax.all_to_all(sums, AXES, split_axis=0, concat_axis=0, tiled=True)
    update, scores = update_of(spread, counts[None, :], columns, chosen)
    return update, scores[0]


def solution(mesh):
    in_specs = (
        P(AXES, None),
        P(AXES, None),
        P("fsdp", None),
        P("fsdp", None),
        P(),
        P(),
        P(),
    )
    return jax.shard_map(
        functools.partial(per_device, mesh.shape["grp"], mesh.shape["fsdp"]),
        mesh=mesh,
        in_specs=in_specs,
        out_specs=(P("fsdp", None), P()),
        check_vma=False,
    )
```
